128 devices in a mesh: dp: 32 (over y, x, core), tp: 4 (over z).
Axes of the slice: x: 4, y: 4, z: 4, core: 2. Of those that a mesh axis runs over, the one named last changes fastest.
Arguments:
- tokens: bfloat16 [16384, 4096], P(('dp', 'tp')), may hold values from -6 to 6
- norm_gain: float32 [4096], replicated, may hold values from 0.1 to 1.9
- w_query: bfloat16 [4096, 4096], P(None, 'tp'), may hold values from -0.09375 to 0.09375
- w_key: bfloat16 [4096, 1024], P(None, 'tp'), may hold values from -2.34375 to 2.34375
- w_value: bfloat16 [4096, 1024], P(None, 'tp'), may hold values from -0.09375 to 0.09375
- w_output: bfloat16 [4096, 4096], P('tp'), may hold values from -0.09375 to 0.09375
- doc_lengths: int32 [128], replicated, may hold values from 1 to 512, as said below
- pack_index: int32 [16384], replicated, may hold values from 0 to 16383, as said below
Outputs:
- output: bfloat16 [16384, 4096], P(('dp', 'tp'))
The draws below stay inside these ranges and needn't reach their ends.
Inputs may be any that keep to these rules, and one draw needn't show every extreme that they name: `doc_lengths`: each run of 4 documents numbered g * 4 to g * 4 + 4 - 1 (the documents of group g) holds at most 1024 tokens together, and some group holds exactly 1024. No document is longer than 512 tokens, and one has exactly that many. `pack_index`: each packed position appears once. The 128 rows of one device hold at most 8 tokens of the documents of any one group; every device holds the same number of one group's tokens, up to one.
All inputs are finite; a program needn't handle non-finite values.
Results may differ from the reference program's by a relative error of at most 0.01.
Values may be sent and summed in bfloat16 or wider, within the bound.
No kernel may reach another device: no remote copies, remote signals or barrier semaphores. Data moves between devices by JAX's collectives and lax.ppermute only.
A program may use at most 128 MiB of HBM per device.

```python
import jax
import jax.numpy as jnp
from jax import lax

D = 4096
HEADS = 32
KV_HEADS = 8
HEAD_DIM = 128
TOK_DEV = 128
GROUP_DOCS = 4
TOKENS = 16384
DOCS = 128
CAP = 1024
N_DP = 32
DEVICES = 128


def query_columns(key):
    return jax.random.truncated_normal(jax.random.fold_in(key, 11), -6.0, 6.0, (D, HEADS * HEAD_DIM), jnp.float32) * D ** (-0.5)


def draw_w_query(key, part):
    return query_columns(key).astype(jnp.bfloat16)


def draw_w_key(key, part):
    own_draw = jax.random.truncated_normal(jax.random.fold_in(key, 13), -6.0, 6.0, (D, KV_HEADS * HEAD_DIM), jnp.float32) * D ** (-0.5)
    return own_draw.astype(jnp.bfloat16)


def layout_plan(key):
    root_random_key = jax.random.fold_in(key, 29)
    complete_random_key, split_random_key, reward_random_key, jitter_random_key, permute_random_key, turning_random_key = jax.random.split(root_random_key, 6)
    full_group = jax.random.randint(complete_random_key, (), 0, N_DP).astype(jnp.int32)
    half_cap = CAP // 2
    cut_points = jnp.sort(jax.random.permutation(split_random_key, half_cap - 1)[:GROUP_DOCS - 2] + 1).astype(jnp.int32)
    fences = jnp.concatenate([jnp.zeros((1,), jnp.int32), cut_points, jnp.full((1,), half_cap, jnp.int32)])
    lesser_lengths = fences[1:] - fences[:-1]
    unrolled = jnp.concatenate([jnp.full((1,), half_cap, jnp.int32), lesser_lengths])
    turning = jax.random.randint(turning_random_key, (), 0, GROUP_DOCS).astype(jnp.int32)
    full_lengths = jnp.roll(unrolled, turning).astype(jnp.int32)
    remaining_documents = (N_DP - 1) * GROUP_DOCS
    spare_capacity = CAP // GROUP_DOCS - 1
    extra_total = TOKENS - CAP - remaining_documents
    extra_reward = jax.random.randint(reward_random_key, (remaining_documents, 1), 0, 4).astype(jnp.int32)
    random_jitter = jax.random.randint(jitter_random_key, (remaining_documents, spare_capacity), 0, 1024).astype(jnp.int32)
    score_values = (extra_reward * 300 + random_jitter) * (remaining_documents * spare_capacity) + jnp.arange(remaining_documents * spare_capacity, dtype=jnp.int32).reshape(remaining_documents, spare_capacity)
    chosen = lax.top_k(score_values.reshape(-1), extra_total)[1].astype(jnp.int32)
    other_lengths = 1 + jax.ops.segment_sum(jnp.ones_like(chosen), chosen // spare_capacity, remaining_documents).astype(jnp.int32)
    slots = jnp.arange(DOCS, dtype=jnp.int32)
    slot_group = slots // GROUP_DOCS
    other_place = jnp.clip(slots - GROUP_DOCS * (slot_group > full_group).astype(jnp.int32), 0, remaining_documents - 1)
    lengths = jnp.where(slot_group == full_group, full_lengths[slots % GROUP_DOCS], other_lengths[other_place]).astype(jnp.int32)
    doc_ends = jnp.cumsum(lengths).astype(jnp.int32)
    doc_starts = doc_ends - lengths
    dealing = jnp.arange(TOKENS, dtype=jnp.int32)
    inside = ((dealing[:, None] >= doc_starts[None, :]) & (dealing[:, None] < doc_ends[None, :])).astype(jnp.int32)
    which_doc = jnp.sum(inside * jnp.arange(DOCS, dtype=jnp.int32)[None, :], axis=1)
    offset = dealing - jnp.sum(inside * doc_starts[None, :], axis=1)
    packed = doc_starts[which_doc] + offset
    dealt = packed.reshape(TOK_DEV, DEVICES).T
    shuffle = jnp.argsort(jax.random.randint(permute_random_key, (DEVICES, TOK_DEV), 0, 1 << 20).astype(jnp.int32) * TOK_DEV + jnp.arange(TOK_DEV, dtype=jnp.int32)[None, :], axis=1)
    placed = jnp.take_along_axis(dealt, shuffle, axis=1).reshape(TOKENS).astype(jnp.int32)
    return (lengths, placed)


def draw_doc_lengths(key, part):
    return layout_plan(key)[0]


def draw_pack_index(key, part):
    return layout_plan(key)[1]


def shard_levels(key, shape, pieces, low, largest):
    def one(axis_at, shards_of):
        heights = jax.random.uniform(jax.random.fold_in(jax.random.fold_in(key, 6), axis_at), (shards_of,), jnp.float32, low / len(pieces), largest / len(pieces))
        return jnp.repeat(jnp.exp(heights), shape[axis_at] // shards_of).reshape((-1,) + (1,) * (len(shape) - axis_at - 1))

    loudness = one(*pieces[0])
    for cut in pieces[1:]:
        loudness = loudness * one(*cut)
    return loudness


def bell_draw(rng, dims, width, bound, cuts=(), held_as=jnp.bfloat16):
    drawn = jax.random.normal(rng, dims, jnp.float32) * width
    if len(cuts) > 0:
        drawn = shard_levels(rng, dims, cuts, -0.22, 0.18) * drawn
    return jnp.clip(drawn, min=-bound, max=bound).astype(held_as)


def setup_inputs(seed: int = 0) -> dict:
    keys = jax.random.split(jax.random.key(seed), 9)
    return {
        "tokens": bell_draw(keys[0], (TOKENS, D), 1.0, 6.0, ((0, 128),)),
        "norm_gain": jnp.clip(1.0 + 0.18 * jax.random.normal(keys[1], (D,), jnp.float32), 0.1, 1.9),
        "w_query": draw_w_query(jax.random.fold_in(keys[8], 71), 0),
        "w_key": draw_w_key(jax.random.fold_in(keys[8], 71), 0),
        "w_value": bell_draw(keys[4], (D, KV_HEADS * HEAD_DIM), D ** -0.5, 0.09375, ((1, 4),)),
        "w_output": bell_draw(keys[5], (HEADS * HEAD_DIM, D), (HEADS * HEAD_DIM) ** -0.5, 0.09375, ((0, 4),)),
        "doc_lengths": draw_doc_lengths(jax.random.fold_in(keys[8], 71), 0),
        "pack_index": draw_pack_index(jax.random.fold_in(keys[8], 71), 0),
    }


rope_base = 500000.0
norm_eps = 1e-05
score_floor = -1e+30

def row_facts(pack_index, doc_lengths):
    doc_ends = jnp.cumsum(doc_lengths).astype(jnp.int32)
    doc_starts = doc_ends - doc_lengths
    inside = ((pack_index[:, None] >= doc_starts[None, :]) & (pack_index[:, None] < doc_ends[None, :])).astype(jnp.int32)
    doc_index = lax.optimization_barrier(jnp.sum(inside * jnp.arange(doc_lengths.shape[0], dtype=jnp.int32)[None, :], axis=1))
    position = pack_index - lax.optimization_barrier(jnp.sum(inside * doc_starts[None, :], axis=1))
    owner_group = (doc_index // GROUP_DOCS).astype(jnp.int32)
    return (doc_index, position, owner_group)

def rotate(projected, position, head_count):
    row_count = projected.shape[0]
    half_dim = HEAD_DIM // 2
    spread = projected.reshape(row_count, head_count, HEAD_DIM)
    frequency = rope_base ** (-2.0 * jnp.arange(half_dim, dtype=jnp.float32) / HEAD_DIM)
    angles = position.astype(jnp.float32)[:, None] * frequency[None, :]
    cosine = jnp.cos(angles)[:, None, :]
    sine = jnp.sin(angles)[:, None, :]
    lower_part = spread[:, :, :half_dim]
    upper_part = spread[:, :, half_dim:]
    turned = jnp.concatenate([lower_part * cosine - upper_part * sine, upper_part * cosine + lower_part * sine], axis=2)
    return turned.reshape(row_count, head_count * HEAD_DIM)

def attend_exact(query, key_rows, value_rows, segment, places):
    slot_total = query.shape[0]
    group_size = HEADS // KV_HEADS
    query_heads = query.astype(jnp.float32).reshape(slot_total, KV_HEADS, group_size, HEAD_DIM)
    key_heads = key_rows.astype(jnp.float32).reshape(slot_total, KV_HEADS, HEAD_DIM)
    value_heads = value_rows.astype(jnp.float32).reshape(slot_total, KV_HEADS, HEAD_DIM)
    score_values = jnp.einsum('qkgd,skd->kgqs', query_heads, key_heads, precision=lax.Precision.HIGHEST) * HEAD_DIM ** (-0.5)
    allowed = (segment[:, None] == segment[None, :]) & (places[None, :] <= places[:, None])
    score_values = jnp.where(allowed[None, None], score_values, score_floor)
    row_peak = lax.optimization_barrier(jnp.max(score_values, axis=-1, keepdims=True))
    weights = jnp.exp(score_values - row_peak)
    weights = (weights / lax.optimization_barrier(jnp.sum(weights, axis=-1, keepdims=True))).astype(jnp.bfloat16)
    mixed_values = jnp.einsum('kgqs,skd->qkgd', weights.astype(jnp.float32), value_heads, precision=lax.Precision.HIGHEST)
    return mixed_values.astype(jnp.bfloat16).reshape(slot_total, HEADS * HEAD_DIM)

def reference(tokens, norm_gain, w_query, w_key, w_value, w_output, doc_lengths, pack_index):
    doc_index, position, owner_group = row_facts(pack_index, doc_lengths)
    residual = tokens.astype(jnp.float32)
    normed = (residual * lax.rsqrt(lax.optimization_barrier(jnp.mean(residual * residual, axis=1, keepdims=True)) + norm_eps) * norm_gain).astype(jnp.bfloat16)
    query = rotate(jnp.dot(normed, w_query, preferred_element_type=jnp.float32), position, HEADS).astype(jnp.bfloat16)
    key_rows = rotate(jnp.dot(normed, w_key, preferred_element_type=jnp.float32), position, KV_HEADS).astype(jnp.bfloat16)
    value_rows = jnp.dot(normed, w_value, preferred_element_type=jnp.float32).astype(jnp.bfloat16)
    ranked = jnp.argsort(owner_group * TOKENS + jnp.arange(TOKENS, dtype=jnp.int32)).astype(jnp.int32)
    counts = jax.ops.segment_sum(jnp.ones((TOKENS,), jnp.int32), owner_group, N_DP).astype(jnp.int32)
    firsts = (jnp.cumsum(counts) - counts).astype(jnp.int32)
    padded = jnp.concatenate([ranked, jnp.zeros((CAP,), jnp.int32)])
    slot_ids = jnp.arange(CAP, dtype=jnp.int32)

    def one_group(gathered, group_id):
        chosen = lax.dynamic_slice_in_dim(padded, firsts[group_id], CAP)
        occupied = slot_ids < counts[group_id]
        segment = jnp.where(occupied, doc_index[chosen], -1 - slot_ids)
        places = jnp.where(occupied, position[chosen], 0)
        context = attend_exact(query[chosen], key_rows[chosen], value_rows[chosen], segment, places)
        target = jnp.where(occupied, chosen, TOKENS)
        return (gathered.at[target].set(context, mode='drop'), None)
    gathered, _ = lax.scan(one_group, jnp.zeros((TOKENS, HEADS * HEAD_DIM), jnp.bfloat16), jnp.arange(N_DP, dtype=jnp.int32))
    attended = jnp.dot(gathered, w_output, preferred_element_type=jnp.float32)
    return (residual + attended).astype(jnp.bfloat16)
```

```python
import functools

import jax
import jax.numpy as jnp
from jax import lax
from jax.experimental import pallas as pl
from jax.experimental.pallas import tpu as pltpu
from jax.sharding import PartitionSpec as P


HEAD_DIM = 128
NY, NX, NZ = 4, 4, 4
GROUPS = 32
TOK = 128
ROWS = NZ * TOK
TILE = 16
TILES = ROWS // TILE
LOG2E = 1.4426950408889634

rope_base = 500000.0
norm_eps = 1e-05
score_floor = -1e30

AXES = ("dp", "tp")
VMEM = pltpu.VMEM


def group_of(y, x, core):
    return ((y % NY) * NX + (x % NX)) * 2 + core


def pairs(move):
    out = []
    for y in range(NY):
        for x in range(NX):
            for core in range(2):
                for z in range(NZ):
                    y2, x2, core2, z2 = move(y, x, core, z)
                    out.append(
                        (group_of(y, x, core) * NZ + z, group_of(y2, x2, core2) * NZ + z2 % NZ)
                    )
    return out


def first_axis(s):
    return pairs(
        lambda y, x, core, z: (y, x + s, core, z) if core == 0 else (y + s, x, core, z)
    )


def second_axis(s):
    return pairs(
        lambda y, x, core, z: (y + s, x, core, z) if core == 0 else (y, x + s, core, z)
    )


def along_z(s):
    return pairs(lambda y, x, core, z: (y, x, core, z + s))


def send(array, moves):
    return lax.ppermute(array, AXES, moves)


def swap_cores(array):
    return send(array, pairs(lambda y, x, core, z: (y, x, 1 - core, z)))


def cost(flops, nbytes, exps=0):
    return pl.CostEstimate(flops=int(flops), bytes_accessed=int(nbytes), transcendentals=int(exps))


def whole():
    return pl.BlockSpec(memory_space=VMEM)


def scalars():
    return pl.BlockSpec(memory_space=pltpu.SMEM)


def small():
    return pltpu.CompilerParams(vmem_limit_bytes=24 * 2**20)


def norm_kernel(tokens_ref, gain_ref, out_ref):
    gain = gain_ref[...]

    def chunk(i, _):
        at = pl.ds(pl.multiple_of(i * 16, 16), 16)
        rows = tokens_ref[at, :].astype(jnp.float32)
        scale = lax.rsqrt(jnp.mean(rows * rows, axis=1, keepdims=True) + norm_eps)
        out_ref[at, :] = (rows * scale * gain).astype(jnp.bfloat16)
        return 0

    lax.fori_loop(0, tokens_ref.shape[0] // 16, chunk, 0)


def normalise(tokens, gain):
    rows, width = tokens.shape
    return pl.pallas_call(
        norm_kernel,
        out_shape=jax.ShapeDtypeStruct((rows, width), jnp.bfloat16),
        in_specs=[whole(), whole()],
        out_specs=whole(),
        compiler_params=small(),
        cost_estimate=cost(rows * width * 5, rows * width * 4),
    )(tokens, gain.reshape(1, width))


def as_column(row):
    return jnp.broadcast_to(row, (128, 128)).T


def order_kernel(packed_ref, out_ref):
    lane = lax.broadcasted_iota(jnp.int32, (128, 128), 1).astype(jnp.float32)
    blocks = ROWS // 128

    def one_group(g, _):
        row = packed_ref[pl.ds(g, 1), :]
        pieces = [row[:, i * 128 : (i + 1) * 128] for i in range(blocks)]
        sums = [jnp.zeros((128, 128), jnp.float32) for _ in range(blocks)]
        for j in range(blocks):
            column = as_column(pieces[j])
            below = jnp.zeros((128, 128), jnp.float32)
            for i in range(blocks):
                below = below + jnp.where(pieces[i] < column, 1.0, 0.0)
            rank = jnp.sum(below, axis=1, keepdims=True)
            for i in range(blocks):
                sums[i] = sums[i] + jnp.where(rank == lane + float(i * 128), column, 0.0)
        out_ref[pl.ds(g, 1), :] = jnp.concatenate(
            [jnp.sum(s, axis=0, keepdims=True) for s in sums], axis=1
        )
        return 0

    lax.fori_loop(0, GROUPS, one_group, 0)


def order_groups(packed):
    return pl.pallas_call(
        order_kernel,
        out_shape=jax.ShapeDtypeStruct((GROUPS, ROWS), jnp.float32),
        in_specs=[whole()],
        out_specs=whole(),
        compiler_params=small(),
        cost_estimate=cost(6 * GROUPS * ROWS * ROWS, 8 * GROUPS * ROWS),
    )(packed)


def turn(head, cosine, sine):
    return head * cosine + pltpu.roll(head, HEAD_DIM // 2, 1) * sine


def stacked(refs):
    if len(refs) == 1:
        return refs[0][...]
    return jnp.concatenate([ref[...] for ref in refs], axis=0)


def keys_and_values(rows, wk_ref, wv_ref, cosine, sine):
    keys = jnp.dot(rows, wk_ref[...], preferred_element_type=jnp.float32)
    values = jnp.dot(rows, wv_ref[...], preferred_element_type=jnp.float32)
    out = []
    for head in range(2):
        at = slice(head * HEAD_DIM, (head + 1) * HEAD_DIM)
        key = turn(keys[:, at], cosine, sine)
        out.append(jnp.concatenate([key, values[:, at]], axis=1).astype(jnp.bfloat16))
    return out


def kv_kernel(parts, first, *refs):
    wk_ref, wv_ref, cos_ref, sin_ref, out_ref = refs[parts:]
    rows = stacked(refs[:parts])
    at = slice(first, first + rows.shape[0])
    for head, block in enumerate(
        keys_and_values(rows, wk_ref, wv_ref, cos_ref[at, :], sin_ref[at, :])
    ):
        out_ref[head] = block


def project_kv(pieces, w_key, w_value, cosine, sine, first):
    width = w_key.shape[0]
    rows = sum(p.shape[0] for p in pieces)
    return pl.pallas_call(
        functools.partial(kv_kernel, len(pieces), first),
        out_shape=jax.ShapeDtypeStruct((2, rows, 256), jnp.bfloat16),
        in_specs=[whole()] * (len(pieces) + 4),
        out_specs=whole(),
        compiler_params=small(),
        cost_estimate=cost(2 * rows * width * 512, width * 1024 + rows * width * 2),
    )(*pieces, w_key, w_value, cosine, sine)


def sorting(rank_row):
    slot = lax.broadcasted_iota(jnp.int32, (ROWS, ROWS), 0)
    return (slot == rank_row).astype(jnp.bfloat16)


def last_kv_kernel(parts, core_ref, *refs):
    wk_ref, wv_ref, cos_ref, sin_ref, rank_ref = refs[parts : parts + 5]
    done_refs, (other_ref, mine_ref) = refs[parts + 5 : -3], refs[-3:-1]
    last_ref = refs[-1]
    rows = stacked(refs[:parts])
    at = slice(ROWS - rows.shape[0], ROWS)
    for head, block in enumerate(
        keys_and_values(rows, wk_ref, wv_ref, cos_ref[at, :], sin_ref[at, :])
    ):
        last_ref[head] = block
    pick = sorting(rank_ref[...])
    core = core_ref[0]
    for head, out_ref in ((1 - core, other_ref), (core, mine_ref)):
        rows = jnp.concatenate([ref[head] for ref in (*done_refs, last_ref)], axis=0)
        out_ref[...] = jnp.dot(pick, rows, preferred_element_type=jnp.float32).astype(jnp.bfloat16)


def finish_kv(core, pieces, w_key, w_value, cosine, sine, rank_row, done):
    width = w_key.shape[0]
    rows = sum(p.shape[0] for p in pieces)
    shape = jax.ShapeDtypeStruct((ROWS, 256), jnp.bfloat16)
    return pl.pallas_call(
        functools.partial(last_kv_kernel, len(pieces)),
        out_shape=(shape, shape),
        in_specs=[scalars()] + [whole()] * (len(pieces) + 5 + len(done)),
        out_specs=(whole(), whole()),
        scratch_shapes=[pltpu.VMEM((2, rows, 256), jnp.bfloat16)],
        compiler_params=small(),
        cost_estimate=cost(2 * rows * width * 512, width * 1024 + rows * width * 2),
    )(core, *pieces, w_key, w_value, cosine, sine, rank_row, *done)


def q_kernel(parts, core_ref, *refs):
    w_ref, cos_ref, sin_ref, rank_ref, other_ref, mine_ref = refs[parts:]
    both = jnp.dot(stacked(refs[:parts]), w_ref[...], preferred_element_type=jnp.float32)
    cosine, sine = cos_ref[...], sin_ref[...]
    turned = jnp.concatenate(
        [turn(both[:, :HEAD_DIM], cosine, sine), turn(both[:, HEAD_DIM:], cosine, sine)], axis=1
    ).astype(jnp.bfloat16)
    ordered = jnp.dot(
        sorting(rank_ref[...]), turned, preferred_element_type=jnp.float32
    ).astype(jnp.bfloat16)
    step = pl.program_id(0)

    @pl.when(step < 2)
    def _():
        other_ref[...] = ordered

    @pl.when(step >= 2)
    def _():
        mine_ref[...] = ordered


def project_q(core, pieces, w_query, cosine, sine, rank_row):
    width = w_query.shape[0]

    def columns(step, core_ref):
        half = jnp.where(step < 2, 1 - core_ref[0], core_ref[0])
        return (0, half * 2 + step % 2)

    shape = jax.ShapeDtypeStruct((ROWS, 512), jnp.bfloat16)
    return pl.pallas_call(
        functools.partial(q_kernel, len(pieces)),
        out_shape=(shape, shape),
        grid_spec=pltpu.PrefetchScalarGridSpec(
            num_scalar_prefetch=1,
            grid=(4,),
            in_specs=[whole()] * len(pieces)
            + [pl.BlockSpec((width, 256), columns)]
            + [whole()] * 3,
            out_specs=(
                pl.BlockSpec((ROWS, 256), lambda i, s: (0, jnp.minimum(i, 1))),
                pl.BlockSpec((ROWS, 256), lambda i, s: (0, jnp.maximum(i - 2, 0))),
            ),
        ),
        compiler_params=small(),
        cost_estimate=cost(2 * ROWS * width * 1024, width * 2048 + ROWS * width * 2),
    )(core, *pieces, w_query, cosine, sine, rank_row)


def attend_kernel(opening, closing, count, low_ref, high_ref, *refs):
    q_refs, refs = refs[:2], refs[2:]
    key_at_ref, row_at_ref, row_from_ref = refs[:3]
    kv_refs, refs = refs[3 : 3 + count], refs[3 + count :]
    if not opening:
        old_ref, refs = refs[0], refs[1:]
    out_refs, state_ref = refs[:-1], refs[-1]
    scale = HEAD_DIM ** (-0.5) * LOG2E

    def at(u, size):
        return pl.ds(pl.multiple_of(u * size, size), size)

    def queries(u):
        query = jnp.concatenate(
            [
                ref[at(u, TILE), h * HEAD_DIM : (h + 1) * HEAD_DIM]
                for ref in q_refs
                for h in range(4)
            ],
            axis=0,
        )
        return (
            query,
            as_column(row_at_ref[pl.ds(u, 1), :]),
            as_column(row_from_ref[pl.ds(u, 1), :]),
        )

    def keys(t):
        return jnp.concatenate(
            [ref[:, at(t, TILE), :].reshape(-1, 256) for ref in kv_refs], axis=0
        )

    def spread(a, wide=1):
        a = jnp.broadcast_to(a, (128, 128))
        return a if wide == 1 else jnp.concatenate([a] * wide, axis=1)

    def update(bound, kv, key_at, state):
        query, upper, lower = bound
        scores = lax.dot_general(
            query,
            kv[:, :HEAD_DIM],
            (((1,), (1,)), ((), ())),
            preferred_element_type=jnp.float32,
        )
        wide = scores.shape[1] // 128
        allowed = (key_at <= spread(upper, wide)) & (key_at >= spread(lower, wide))
        scores = jnp.where(allowed, scores, score_floor)
        peak = spread(jnp.max(scores, axis=1, keepdims=True))
        if state is not None:
            peak = jnp.maximum(peak, state[0])
        weights = jnp.exp2((scores - spread(peak, wide)) * scale)
        total = spread(jnp.sum(weights, axis=1, keepdims=True))
        mixed = jnp.dot(
            weights.astype(jnp.bfloat16), kv[:, HEAD_DIM:], preferred_element_type=jnp.float32
        )
        if state is not None:
            keep = jnp.exp2((state[0] - peak) * scale)
            total = total + state[1] * keep
            mixed = mixed + state[2] * keep
        return peak, total, mixed

    def load(ref, u):
        return tuple(ref[at(u, 128), i * 128 : (i + 1) * 128] for i in range(3))

    def save(u, state):
        for i, part in enumerate(state):
            state_ref[at(u, 128), i * 128 : (i + 1) * 128] = part

    def write(u, state):
        _, total, mixed = state
        context = (mixed / total).astype(jnp.bfloat16)
        for i, ref in enumerate(out_refs):
            for h in range(4):
                block = (i * 4 + h) * TILE
                ref[at(u, TILE), h * HEAD_DIM : (h + 1) * HEAD_DIM] = context[block : block + TILE]

    def start(u):
        low, high = low_ref[u], high_ref[u]
        t0 = jnp.minimum(low, TILES - 1)
        t1 = jnp.minimum(low + 1, TILES - 1)
        at0 = jnp.where(low < high, key_at_ref[pl.ds(t0, 1), :], -1.0)
        at1 = jnp.where(low + 1 < high, key_at_ref[pl.ds(t1, 1), :], -1.0)
        kv = jnp.concatenate([keys(t0), keys(t1)], axis=0)
        state = None if opening else load(old_ref, u)
        state = update(queries(u), kv, jnp.concatenate([at0, at1], axis=1), state)
        save(u, state)
        if closing:
            write(u, state)

    def two(i, _):
        start(2 * i)
        start(2 * i + 1)
        return 0

    lax.fori_loop(0, TILES // 2, two, 0)

    def rest(u, _):
        def more(t, _):
            state = update(
                queries(u), keys(t), key_at_ref[pl.ds(t, 1), :], load(state_ref, u)
            )
            save(u, state)
            if closing:
                write(u, state)
            return 0

        return lax.fori_loop(low_ref[u] + 2, high_ref[u], more, 0)

    lax.fori_loop(0, TILES, rest, 0)


def attend(bounds, queries, key_at, rows_bounds, kvs, state, closing):
    opening = state is None
    running = jax.ShapeDtypeStruct((TILES * 128, 384), jnp.float32)
    context = [jax.ShapeDtypeStruct((ROWS, 512), jnp.bfloat16)] * 2
    operands = [*bounds, *queries, key_at, *rows_bounds, *kvs, *(() if opening else (state,))]
    rows = sum(kv.shape[0] for kv in kvs) * TILE * 2
    return pl.pallas_call(
        functools.partial(attend_kernel, opening, closing, len(kvs)),
        out_shape=context if closing else running,
        in_specs=[scalars(), scalars()] + [whole()] * (len(operands) - 2),
        out_specs=[whole()] * 2 if closing else whole(),
        scratch_shapes=[pltpu.VMEM((TILES * 128, 384), jnp.float32)] if closing else (),
        compiler_params=pltpu.CompilerParams(vmem_limit_bytes=32 * 2**20),
        cost_estimate=cost(TILES * 128 * rows * 512, 10e6, TILES * 128 * rows),
    )(*operands)


def unsort(rank_row, block, parts):
    slot = lax.broadcasted_iota(jnp.int32, (TOK, ROWS), 1)
    rank = as_column(rank_row[:, block * TOK : (block + 1) * TOK])
    pick = (slot == jnp.concatenate([rank] * (ROWS // 128), axis=1)).astype(jnp.bfloat16)
    return [
        jnp.dot(pick, part[...], preferred_element_type=jnp.float32).astype(jnp.bfloat16)
        for part in parts
    ]


def product_kernel(wanted, core_ref, rank_ref, mine_ref, other_ref, w_ref, *out_refs):
    core = core_ref[0]
    mine_at = pl.ds(pl.multiple_of(core * 512, 512), 512)
    other_at = pl.ds(pl.multiple_of((1 - core) * 512, 512), 512)
    half = w_ref.shape[1] // 2
    rank = rank_ref[...]
    rows = {}
    for block, side in wanted:
        if block not in rows:
            rows[block] = unsort(rank, block, (mine_ref, other_ref))
    for side in range(2):
        group = [(i, block) for i, (block, s) in enumerate(wanted) if s == side]
        mine = jnp.concatenate([rows[block][0] for _, block in group], axis=0)
        other = jnp.concatenate([rows[block][1] for _, block in group], axis=0)
        for at in range(side * half, (side + 1) * half, 1024):
            product = jnp.dot(
                mine, w_ref[mine_at, at : at + 1024], preferred_element_type=jnp.float32
            ) + jnp.dot(other, w_ref[other_at, at : at + 1024], preferred_element_type=jnp.float32)
            for n, (i, _) in enumerate(group):
                out_refs[i][:, at - side * half : at - side * half + 1024] = product[
                    n * TOK : (n + 1) * TOK
                ].astype(jnp.bfloat16)


def products(core, rank_row, mine, other, w_output, wanted):
    width = w_output.shape[1]
    shape = jax.ShapeDtypeStruct((TOK, width // 2), jnp.bfloat16)
    return pl.pallas_call(
        functools.partial(product_kernel, wanted),
        out_shape=[shape] * len(wanted),
        in_specs=[scalars()] + [whole()] * 4,
        out_specs=[whole()] * len(wanted),
        compiler_params=small(),
        cost_estimate=cost(TOK * 1024 * width * len(wanted), 1024 * width * 2),
    )(core, rank_row, mine, other, w_output)


def document_start(position, starts):
    reached = starts <= position[..., None]
    return jnp.max(jnp.where(reached, starts, 0), axis=-1)


def layer(tokens, norm_gain, w_query, w_key, w_value, w_output, doc_lengths, pack_index):
    group = lax.axis_index("dp")
    z = lax.axis_index("tp")
    core = group % 2
    chip_x = (group // 2) % NX
    chip_y = group // (2 * NX)
    core_arg = core.astype(jnp.int32).reshape(1)

    normed = normalise(tokens, norm_gain)
    below = send(normed, along_z(1))
    above = send(normed, along_z(-1))
    far_low = send(below[: TOK // 2], along_z(1))
    far_high = send(above[TOK // 2 :], along_z(-1))

    number = jnp.arange(doc_lengths.shape[0], dtype=jnp.int32)
    starts = jnp.sum(jnp.where(number[None, :] < number[:, None], doc_lengths[None, :], 0), axis=1)
    by_group = pack_index.reshape(GROUPS, NZ, TOK)
    own = lax.dynamic_index_in_dim(by_group, group, 0, keepdims=False)
    order = (z + jnp.array([0, NZ - 1, 1, 2], jnp.int32)) % NZ
    packed = jnp.take(own, order, axis=0).reshape(ROWS)
    place = packed - document_start(packed, starts)
    rank_row = jnp.sum((packed[:, None] < packed[None, :]).astype(jnp.int32), axis=0)
    rank_row = rank_row.reshape(1, ROWS)
    half_dim = HEAD_DIM // 2
    frequency = rope_base ** (-2.0 * jnp.arange(half_dim, dtype=jnp.float32) / HEAD_DIM)
    angles = place.astype(jnp.float32)[:, None] * frequency[None, :]
    cosine, sine = jnp.cos(angles), jnp.sin(angles)
    cosine = jnp.concatenate([cosine, cosine], axis=1)
    sine = jnp.concatenate([-sine, sine], axis=1)

    kv_own = project_kv((normed,), w_key, w_value, cosine, sine, 0)
    kv_near = project_kv((below, above), w_key, w_value, cosine, sine, TOK)
    kv_other, kv_mine = finish_kv(
        core_arg, (far_low, far_high), w_key, w_value, cosine, sine, rank_row, (kv_own, kv_near)
    )
    kv_partner = swap_cores(kv_other)
    chip = jnp.concatenate([kv_mine[None], kv_partner[None]], axis=0)

    back = send(chip, first_axis(1))
    ahead = send(chip, first_axis(-1))
    far_a = send(back[:1], first_axis(1))
    far_b = send(ahead[1:], first_axis(-1))
    line_a = jnp.concatenate([chip, back], axis=0)
    a_back = send(line_a, second_axis(1))
    a_ahead = send(line_a, second_axis(-1))
    line_b = jnp.concatenate([ahead, far_a, far_b], axis=0)
    b_ahead = send(line_b, second_axis(-1))
    b_back = send(line_b, second_axis(1))
    a_far = send(a_back, second_axis(1))
    b_far = send(b_ahead, second_axis(-1))

    q_other, q_mine = project_q(
        core_arg, (normed, below, above, far_low, far_high), w_query, cosine, sine, rank_row
    )
    q_partner = swap_cores(q_other)
    queries = (q_mine, q_partner)

    ordered = order_groups(pack_index.reshape(GROUPS, ROWS).astype(jnp.float32))
    offsets = jnp.array([0, -1, 1, 2], jnp.int32)
    outer, inner = offsets[:, None, None], offsets[None, :, None]
    which = (core + jnp.arange(2, dtype=jnp.int32)) % 2
    dy = jnp.where(core == 0, outer, inner)
    dx = jnp.where(core == 0, inner, outer)
    source = (((chip_y + dy) % NY) * NX + (chip_x + dx) % NX) * 2 + which[None, None, :]
    key_at = jnp.take(ordered, source.reshape(GROUPS), axis=0)
    key_at = key_at.reshape(GROUPS, TILES, TILE).transpose(1, 0, 2)
    rows_at = jnp.take(ordered, jnp.stack([group, group + 1 - 2 * core]), axis=0)
    rows_from = document_start(rows_at, starts.astype(jnp.float32))
    rows_at = rows_at.reshape(2, TILES, TILE)
    rows_from = rows_from.reshape(2, TILES, TILE)
    first_needed = jnp.min(rows_from, axis=(0, 2))
    last_needed = jnp.max(rows_at, axis=(0, 2))

    def per_row(a):
        a = jnp.broadcast_to(a.transpose(1, 0, 2)[:, :, None, :], (TILES, 2, 4, TILE))
        return a.reshape(TILES, 128)

    rows_bounds = (per_row(rows_at), per_row(rows_from))
    state = None
    for name, first, count, kvs in (
        ("att_one", 0, 8, (line_a, line_b)),
        ("att_two", 8, 16, (a_back, b_back, a_ahead, b_ahead)),
        ("att_end", 24, 8, (a_far, b_far)),
    ):
        part = key_at[:, first : first + count].reshape(TILES, count * TILE)
        tile_first = jnp.min(part, axis=1)
        tile_last = jnp.max(part, axis=1)
        low = jnp.sum((tile_last[None, :] < first_needed[:, None]).astype(jnp.int32), axis=1)
        high = jnp.sum((tile_first[None, :] <= last_needed[:, None]).astype(jnp.int32), axis=1)
        state = attend(
            (low, high), queries, part, rows_bounds, kvs, state, name == "att_end"
        )
    mine, partner = state
    other = swap_cores(partner)

    p, q = products(core_arg, rank_row, mine, other, w_output, ((1, 0), (2, 1)))
    p, q = send(p, along_z(1)), send(q, along_z(-1))
    p1, q1, p2, q2, p3, q3 = products(
        core_arg,
        rank_row,
        mine,
        other,
        w_output,
        ((3, 0), (3, 1), (2, 0), (1, 1), (0, 0), (0, 1)),
    )

    def plus(a, b):
        return a.astype(jnp.float32) + b.astype(jnp.float32)

    p = send(plus(p, p1).astype(jnp.bfloat16), along_z(1))
    q = send(plus(q, q1).astype(jnp.bfloat16), along_z(-1))
    p = send(plus(p, p2).astype(jnp.bfloat16), along_z(1))
    q = send(plus(q, q2).astype(jnp.bfloat16), along_z(-1))
    attended = jnp.concatenate([plus(p, p3), plus(q, q3)], axis=1)
    return (tokens.astype(jnp.float32) + attended).astype(jnp.bfloat16)


def solution(mesh):
    placed = (
        P(("dp", "tp"), None),
        P(),
        P(None, "tp"),
        P(None, "tp"),
        P(None, "tp"),
        P("tp", None),
        P(),
        P(),
    )
    return jax.shard_map(
        layer, mesh=mesh, in_specs=placed, out_specs=P(("dp", "tp"), None), check_vma=False
    )
```

```python
import functools

import jax
import jax.numpy as jnp
from jax import lax
from jax.experimental import pallas as pl
from jax.experimental.pallas import tpu as pltpu
from jax.sharding import PartitionSpec as P


HEAD_DIM = 128
NY, NX, NZ = 4, 4, 4
GROUPS = 32
TOK = 128
ROWS = NZ * TOK
TILE = 16
SPAN_BITS = 9
TILES = ROWS // TILE
LOG2E = 1.4426950408889634

rope_base = 500000.0
norm_eps = 1e-05
score_floor = -1e30

AXES = ("dp", "tp")
VMEM = pltpu.VMEM


def group_of(y, x, core):
    return ((y % NY) * NX + (x % NX)) * 2 + core


def pairs(move):
    out = []
    for y in range(NY):
        for x in range(NX):
            for core in range(2):
                for z in range(NZ):
                    y2, x2, core2, z2 = move(y, x, core, z)
                    out.append(
                        (group_of(y, x, core) * NZ + z, group_of(y2, x2, core2) * NZ + z2 % NZ)
                    )
    return out


def first_axis(s):
    return pairs(
        lambda y, x, core, z: (y, x + s, core, z) if core == 0 else (y + s, x, core, z)
    )


def second_axis(s):
    return pairs(
        lambda y, x, core, z: (y + s, x, core, z) if core == 0 else (y, x + s, core, z)
    )


def along_z(s):
    return pairs(lambda y, x, core, z: (y, x, core, z + s))


def send(array, moves):
    return lax.ppermute(array, AXES, moves)


def swap_cores(array):
    return send(array, pairs(lambda y, x, core, z: (y, x, 1 - core, z)))


def cost(flops, nbytes, exps=0):
    return pl.CostEstimate(flops=int(flops), bytes_accessed=int(nbytes), transcendentals=int(exps))


def whole():
    return pl.BlockSpec(memory_space=VMEM)


def scalars():
    return pl.BlockSpec(memory_space=pltpu.SMEM)


def small():
    return pltpu.CompilerParams(vmem_limit_bytes=8 * 2**20)


def norm_kernel(tokens_ref, gain_ref, low_ref, high_ref):
    gain = gain_ref[...]
    half = low_ref.shape[0]

    for first, out_ref in ((0, low_ref), (half, high_ref)):

        def chunk(i, _):
            at = pl.multiple_of(i * 16, 16)
            rows = tokens_ref[pl.ds(first + at, 16), :].astype(jnp.float32)
            scale = lax.rsqrt(jnp.mean(rows * rows, axis=1, keepdims=True) + norm_eps)
            out_ref[pl.ds(at, 16), :] = (rows * scale * gain).astype(jnp.bfloat16)
            return 0

        lax.fori_loop(0, half // 16, chunk, 0)


def normalise(tokens, gain):
    rows, width = tokens.shape
    return pl.pallas_call(
        norm_kernel,
        out_shape=[jax.ShapeDtypeStruct((rows // 2, width), jnp.bfloat16)] * 2,
        in_specs=[whole(), whole()],
        out_specs=[whole(), whole()],
        compiler_params=small(),
        cost_estimate=cost(rows * width * 5, rows * width * 4),
    )(tokens, gain.reshape(1, width))


def as_column(row):
    return jnp.broadcast_to(row, (128, 128)).T


def order_kernel(packed_ref, out_ref):
    lane = lax.broadcasted_iota(jnp.int32, (128, 128), 1).astype(jnp.float32)
    blocks = ROWS // 128

    def one_group(g, _):
        row = packed_ref[pl.ds(g, 1), :]
        pieces = [row[:, i * 128 : (i + 1) * 128] for i in range(blocks)]
        sums = [jnp.zeros((128, 128), jnp.float32) for _ in range(blocks)]
        for j in range(blocks):
            column = as_column(pieces[j])
            below = jnp.zeros((128, 128), jnp.float32)
            for i in range(blocks):
                below = below + jnp.where(pieces[i] < column, 1.0, 0.0)
            rank = jnp.sum(below, axis=1, keepdims=True)
            for i in range(blocks):
                sums[i] = sums[i] + jnp.where(rank == lane + float(i * 128), column, 0.0)
        out_ref[pl.ds(g, 1), :] = jnp.concatenate(
            [jnp.sum(s, axis=0, keepdims=True) for s in sums], axis=1
        )
        return 0

    lax.fori_loop(0, GROUPS, one_group, 0)


def order_groups(packed):
    return pl.pallas_call(
        order_kernel,
        out_shape=jax.ShapeDtypeStruct((GROUPS, ROWS), jnp.float32),
        in_specs=[whole()],
        out_specs=whole(),
        compiler_params=small(),
        cost_estimate=cost(6 * GROUPS * ROWS * ROWS, 8 * GROUPS * ROWS),
    )(packed)


def column_kernel(packed_ref, out_ref):
    def one(u, _):
        at = pl.ds(pl.multiple_of(u * 128, 128), 128)
        out_ref[at, :] = as_column(packed_ref[pl.ds(u, 1), :])
        return 0

    lax.fori_loop(0, TILES, one, 0)


def columns_of(packed):
    return pl.pallas_call(
        column_kernel,
        out_shape=jax.ShapeDtypeStruct((TILES * 128, 128), jnp.int32),
        in_specs=[whole()],
        out_specs=whole(),
        compiler_params=small(),
        cost_estimate=cost(TILES * 128 * 128 * 32, TILES * 128 * 512),
    )(packed)


def turn(head, cosine, sine):
    return head * cosine + pltpu.roll(head, HEAD_DIM // 2, 1) * sine


def stacked(refs):
    if len(refs) == 1:
        return refs[0][...]
    return jnp.concatenate([ref[...] for ref in refs], axis=0)


def keys_and_values(rows, wk_ref, wv_ref, cosine, sine):
    keys = jnp.dot(rows, wk_ref[...], preferred_element_type=jnp.float32)
    values = jnp.dot(rows, wv_ref[...], preferred_element_type=jnp.float32)
    out = []
    for head in range(2):
        at = slice(head * HEAD_DIM, (head + 1) * HEAD_DIM)
        key = turn(keys[:, at], cosine, sine)
        out.append(jnp.concatenate([key, values[:, at]], axis=1).astype(jnp.bfloat16))
    return out


def kv_kernel(parts, first, *refs):
    wk_ref, wv_ref, cos_ref, sin_ref, out_ref = refs[parts:]
    rows = stacked(refs[:parts])
    at = slice(first, first + rows.shape[0])
    for head, block in enumerate(
        keys_and_values(rows, wk_ref, wv_ref, cos_ref[at, :], sin_ref[at, :])
    ):
        out_ref[head] = block


def project_kv(pieces, w_key, w_value, cosine, sine, first):
    width = w_key.shape[0]
    rows = sum(p.shape[0] for p in pieces)
    return pl.pallas_call(
        functools.partial(kv_kernel, len(pieces), first),
        out_shape=jax.ShapeDtypeStruct((2, rows, 256), jnp.bfloat16),
        in_specs=[whole()] * (len(pieces) + 4),
        out_specs=whole(),
        compiler_params=small(),
        cost_estimate=cost(2 * rows * width * 512, width * 1024 + rows * width * 2),
    )(*pieces, w_key, w_value, cosine, sine)


def sorting(rank_row):
    slot = lax.broadcasted_iota(jnp.int32, (ROWS, ROWS), 0)
    return (slot == rank_row).astype(jnp.bfloat16)


def last_kv_kernel(parts, core_ref, *refs):
    wk_ref, wv_ref, cos_ref, sin_ref, rank_ref = refs[parts : parts + 5]
    done_refs, (other_ref, mine_ref) = refs[parts + 5 : -3], refs[-3:-1]
    last_ref = refs[-1]
    rows = stacked(refs[:parts])
    at = slice(ROWS - rows.shape[0], ROWS)
    for head, block in enumerate(
        keys_and_values(rows, wk_ref, wv_ref, cos_ref[at, :], sin_ref[at, :])
    ):
        last_ref[head] = block
    pick = sorting(rank_ref[...])
    core = core_ref[0]
    for head, out_ref in ((1 - core, other_ref), (core, mine_ref)):
        rows = jnp.concatenate([ref[head] for ref in (*done_refs, last_ref)], axis=0)
        out_ref[...] = jnp.dot(pick, rows, preferred_element_type=jnp.float32).astype(jnp.bfloat16)


def finish_kv(core, pieces, w_key, w_value, cosine, sine, rank_row, done):
    width = w_key.shape[0]
    rows = sum(p.shape[0] for p in pieces)
    shape = jax.ShapeDtypeStruct((ROWS, 256), jnp.bfloat16)
    return pl.pallas_call(
        functools.partial(last_kv_kernel, len(pieces)),
        out_shape=(shape, shape),
        in_specs=[scalars()] + [whole()] * (len(pieces) + 5 + len(done)),
        out_specs=(whole(), whole()),
        scratch_shapes=[pltpu.VMEM((2, rows, 256), jnp.bfloat16)],
        compiler_params=small(),
        cost_estimate=cost(2 * rows * width * 512, width * 1024 + rows * width * 2),
    )(core, *pieces, w_key, w_value, cosine, sine, rank_row, *done)


def q_kernel(parts, mine, core_ref, *refs):
    w_ref, cos_ref, sin_ref, rank_ref, out_ref, turned_ref = refs[parts:]
    half = core_ref[0] if mine else 1 - core_ref[0]
    for block in range(NZ):
        rows = stacked(refs[2 * block : 2 * block + 2])
        at = slice(block * TOK, (block + 1) * TOK)
        cosine, sine = cos_ref[at, :], sin_ref[at, :]
        for first in range(0, 512, 256):
            columns = pl.ds(pl.multiple_of(half * 512 + first, 256), 256)
            both = jnp.dot(rows, w_ref[:, columns], preferred_element_type=jnp.float32)
            turned = jnp.concatenate(
                [turn(both[:, :HEAD_DIM], cosine, sine), turn(both[:, HEAD_DIM:], cosine, sine)],
                axis=1,
            )
            turned_ref[at, first : first + 256] = (
                turned * (HEAD_DIM ** (-0.5) * LOG2E)
            ).astype(jnp.bfloat16)
    out_ref[...] = jnp.dot(
        sorting(rank_ref[...]), turned_ref[...], preferred_element_type=jnp.float32
    ).astype(jnp.bfloat16)


def project_q(core, pieces, w_query, cosine, sine, rank_row, mine):
    width = w_query.shape[0]
    return pl.pallas_call(
        functools.partial(q_kernel, len(pieces), mine),
        out_shape=jax.ShapeDtypeStruct((ROWS, 512), jnp.bfloat16),
        in_specs=[scalars()] + [whole()] * (len(pieces) + 4),
        out_specs=whole(),
        scratch_shapes=[pltpu.VMEM((ROWS, 512), jnp.bfloat16)],
        compiler_params=small(),
        cost_estimate=cost(2 * ROWS * width * 512, width * 1024 + ROWS * width * 2),
    )(core, *pieces, w_query, cosine, sine, rank_row)


def attend_kernel(opening, closing, batch, count, low_ref, high_ref, *refs):
    q_refs, refs = refs[:2], refs[2:]
    key_at_ref, bound_ref = refs[:2]
    kv_refs, refs = refs[2 : 2 + count], refs[2 + count :]
    if not opening:
        old_ref, refs = refs[0], refs[1:]
    if closing:
        w_from, out_refs, (w_to, state_ref, arrived) = refs[0], refs[1:3], refs[3:]
        copy = pltpu.make_async_copy(w_from, w_to, arrived)
        copy.start()
    else:
        (state_ref,) = refs

    def at(u, size):
        return pl.ds(pl.multiple_of(u * size, size), size)

    def queries(u):
        return jnp.concatenate(
            [
                ref[at(u, TILE), h * HEAD_DIM : (h + 1) * HEAD_DIM]
                for ref in q_refs
                for h in range(4)
            ],
            axis=0,
        )

    def keys(t):
        return jnp.concatenate(
            [ref[:, at(t, TILE), :].reshape(-1, 256) for ref in kv_refs], axis=0
        )

    def spread(a, wide=1):
        a = jnp.broadcast_to(a, (128, 128))
        return a if wide == 1 else jnp.concatenate([a] * wide, axis=1)

    def update(us, kvs, key_ats, states):
        wide = kvs[0].shape[0] // 128
        scores = [
            lax.dot_general(
                queries(u),
                kv[:, :HEAD_DIM],
                (((1,), (1,)), ((), ())),
                preferred_element_type=jnp.float32,
            )
            for u, kv in zip(us, kvs)
        ]
        masked = []
        for u, score, key_at in zip(us, scores, key_ats):
            bound = bound_ref[at(u, 128), :]
            upper = bound >> SPAN_BITS
            lower = upper - (bound & (2**SPAN_BITS - 1))
            allowed = (key_at <= spread(upper, wide)) & (key_at >= spread(lower, wide))
            masked.append(jnp.where(allowed, score, score_floor))
        peaks = [spread(jnp.max(m, axis=1, keepdims=True)) for m in masked]
        peaks = [p if st is None else jnp.maximum(p, st[0]) for p, st in zip(peaks, states)]
        weights = [jnp.exp2(m - spread(p, wide)) for m, p in zip(masked, peaks)]
        totals = [spread(jnp.sum(w, axis=1, keepdims=True)) for w in weights]
        mixes = [
            jnp.dot(w.astype(jnp.bfloat16), kv[:, HEAD_DIM:], preferred_element_type=jnp.float32)
            for w, kv in zip(weights, kvs)
        ]
        out = []
        for peak, total, mixed, st in zip(peaks, totals, mixes, states):
            if st is not None:
                keep = jnp.exp2(st[0] - peak)
                total = total + st[1] * keep
                mixed = mixed + st[2] * keep
            out.append((peak, total, mixed))
        return out

    def load(ref, u):
        return tuple(ref[at(u, 128), i * 128 : (i + 1) * 128] for i in range(3))

    def save(u, state):
        for i, part in enumerate(state):
            state_ref[at(u, 128), i * 128 : (i + 1) * 128] = part

    def write(u, state):
        _, total, mixed = state
        context = (mixed / total).astype(jnp.bfloat16)
        for i, ref in enumerate(out_refs):
            for h in range(4):
                block = (i * 4 + h) * TILE
                ref[at(u, TILE), h * HEAD_DIM : (h + 1) * HEAD_DIM] = context[block : block + TILE]

    def finish(us, states):
        for u, state in zip(us, states):
            save(u, state)
            if closing:
                write(u, state)

    def some(i, _):
        us = [batch * i + n for n in range(batch)]
        kvs, key_ats = [], []
        for u in us:
            low, high = low_ref[u], high_ref[u]
            t0 = jnp.minimum(low, TILES - 1)
            t1 = jnp.minimum(low + 1, TILES - 1)
            at0 = jnp.where(low < high, key_at_ref[pl.ds(t0, 1), :], -1)
            at1 = jnp.where(low + 1 < high, key_at_ref[pl.ds(t1, 1), :], -1)
            kvs.append(jnp.concatenate([keys(t0), keys(t1)], axis=0))
            key_ats.append(jnp.concatenate([at0, at1], axis=1))
        states = [None if opening else load(old_ref, u) for u in us]
        finish(us, update(us, kvs, key_ats, states))
        return 0

    lax.fori_loop(0, TILES // batch, some, 0)

    def rest(u, _):
        def more(t, _):
            key_at = key_at_ref[pl.ds(t, 1), :]
            finish([u], update([u], [keys(t)], [key_at], [load(state_ref, u)]))
            return 0

        return lax.fori_loop(low_ref[u] + 2, high_ref[u], more, 0)

    lax.fori_loop(0, TILES, rest, 0)
    if closing:
        copy.wait()


def attend(bounds, queries, key_at, row_bounds, kvs, state, batch, resident=None):
    opening, closing = state is None, resident is not None
    running = jax.ShapeDtypeStruct((TILES * 128, 384), jnp.float32)
    operands = [*bounds, *queries, key_at, row_bounds, *kvs, *(() if opening else (state,))]
    in_specs = [scalars(), scalars()] + [whole()] * (len(operands) - 2)
    out_shape, out_specs, scratch = running, whole(), ()
    if closing:
        operands.append(resident)
        in_specs.append(pl.BlockSpec(memory_space=pltpu.HBM))
        context = jax.ShapeDtypeStruct((ROWS, 512), jnp.bfloat16)
        out_shape = [context, context, jax.ShapeDtypeStruct(resident.shape, resident.dtype)]
        out_specs = [whole()] * 3
        scratch = [pltpu.VMEM((TILES * 128, 384), jnp.float32), pltpu.SemaphoreType.DMA]
    rows = sum(kv.shape[0] for kv in kvs) * TILE * 2
    return pl.pallas_call(
        functools.partial(attend_kernel, opening, closing, batch, len(kvs)),
        out_shape=out_shape,
        in_specs=in_specs,
        out_specs=out_specs,
        scratch_shapes=scratch,
        compiler_params=pltpu.CompilerParams(vmem_limit_bytes=(29 if closing else 8) * 2**20),
        cost_estimate=cost(TILES * 128 * rows * 512, 10e6, TILES * 128 * rows),
    )(*operands)


def unsort(rank_row, block, parts):
    slot = lax.broadcasted_iota(jnp.int32, (TOK, ROWS), 1)
    rank = as_column(rank_row[:, block * TOK : (block + 1) * TOK])
    pick = (slot == jnp.concatenate([rank] * (ROWS // 128), axis=1)).astype(jnp.bfloat16)
    return [
        jnp.dot(pick, part[...], preferred_element_type=jnp.float32).astype(jnp.bfloat16)
        for part in parts
    ]


def product_kernel(wanted, core_ref, rank_ref, mine_ref, other_ref, w_ref, *out_refs):
    core = core_ref[0]
    mine_at = pl.ds(pl.multiple_of(core * 512, 512), 512)
    other_at = pl.ds(pl.multiple_of((1 - core) * 512, 512), 512)
    part = w_ref.shape[1] // 4
    rank = rank_ref[...]
    rows = {}
    for block, _ in wanted:
        if block not in rows:
            rows[block] = unsort(rank, block, (mine_ref, other_ref))
    for side in range(4):
        group = [(i, block) for i, (block, s) in enumerate(wanted) if s == side]
        mine = jnp.concatenate([rows[block][0] for _, block in group], axis=0)
        other = jnp.concatenate([rows[block][1] for _, block in group], axis=0)
        at = slice(side * part, (side + 1) * part)
        product = jnp.dot(
            mine, w_ref[mine_at, at], preferred_element_type=jnp.float32
        ) + jnp.dot(other, w_ref[other_at, at], preferred_element_type=jnp.float32)
        for n, (i, _) in enumerate(group):
            out_refs[i][...] = product[n * TOK : (n + 1) * TOK].astype(jnp.bfloat16)


def products(core, rank_row, mine, other, w_output, wanted):
    width = w_output.shape[1]
    shape = jax.ShapeDtypeStruct((TOK, width // 4), jnp.bfloat16)
    return pl.pallas_call(
        functools.partial(product_kernel, wanted),
        out_shape=[shape] * len(wanted),
        in_specs=[scalars()] + [whole()] * 4,
        out_specs=[whole()] * len(wanted),
        compiler_params=small(),
        cost_estimate=cost(TOK * 512 * width * len(wanted), 1024 * width * 2),
    )(core, rank_row, mine, other, w_output)


def document_start(position, starts):
    reached = starts <= position[..., None]
    return jnp.max(jnp.where(reached, starts, 0), axis=-1)


def layer(tokens, norm_gain, w_query, w_key, w_value, w_output, doc_lengths, pack_index):
    group = lax.axis_index("dp")
    z = lax.axis_index("tp")
    core = group % 2
    chip_x = (group // 2) % NX
    chip_y = group // (2 * NX)
    core_arg = core.astype(jnp.int32).reshape(1)

    own_low, own_high = normalise(tokens, norm_gain)
    below_low = send(own_low, along_z(1))
    above_high = send(own_high, along_z(-1))
    below_high = send(own_high, along_z(1))
    above_low = send(own_low, along_z(-1))
    far_low = send(below_low, along_z(1))
    far_high = send(above_high, along_z(-1))
    own_rows = (own_low, own_high)
    near_rows = (below_low, below_high, above_low, above_high)
    far_rows = (far_low, far_high)

    number = jnp.arange(doc_lengths.shape[0], dtype=jnp.int32)
    starts = jnp.sum(jnp.where(number[None, :] < number[:, None], doc_lengths[None, :], 0), axis=1)
    by_group = pack_index.reshape(GROUPS, NZ, TOK)
    own = lax.dynamic_index_in_dim(by_group, group, 0, keepdims=False)
    order = (z + jnp.array([0, NZ - 1, 1, 2], jnp.int32)) % NZ
    packed = jnp.take(own, order, axis=0).reshape(ROWS)
    place = packed - document_start(packed, starts)
    rank_row = jnp.sum((packed[:, None] < packed[None, :]).astype(jnp.int32), axis=0)
    rank_row = rank_row.reshape(1, ROWS)
    half_dim = HEAD_DIM // 2
    frequency = rope_base ** (-2.0 * jnp.arange(half_dim, dtype=jnp.float32) / HEAD_DIM)
    angles = place.astype(jnp.float32)[:, None] * frequency[None, :]
    cosine, sine = jnp.cos(angles), jnp.sin(angles)
    cosine = jnp.concatenate([cosine, cosine], axis=1)
    sine = jnp.concatenate([-sine, sine], axis=1)

    kv_own = project_kv(own_rows, w_key, w_value, cosine, sine, 0)

    ordered = order_groups(pack_index.reshape(GROUPS, ROWS).astype(jnp.float32))
    ordered = ordered.astype(jnp.int32)
    offsets = jnp.array([0, -1, 1, 2], jnp.int32)
    outer, inner = offsets[:, None, None], offsets[None, :, None]
    which = (core + jnp.arange(2, dtype=jnp.int32)) % 2
    dy = jnp.where(core == 0, outer, inner)
    dx = jnp.where(core == 0, inner, outer)
    source = (((chip_y + dy) % NY) * NX + (chip_x + dx) % NX) * 2 + which[None, None, :]
    key_at = jnp.take(ordered, source.reshape(GROUPS), axis=0)
    key_at = key_at.reshape(GROUPS, TILES, TILE).transpose(1, 0, 2)
    rows_at = jnp.take(ordered, jnp.stack([group, group + 1 - 2 * core]), axis=0)
    rows_from = document_start(rows_at, starts)
    rows_at = rows_at.reshape(2, TILES, TILE)
    rows_from = rows_from.reshape(2, TILES, TILE)
    first_needed = jnp.min(rows_from, axis=(0, 2))
    last_needed = jnp.max(rows_at, axis=(0, 2))

    def per_row(a):
        a = jnp.broadcast_to(a.transpose(1, 0, 2)[:, :, None, :], (TILES, 2, 4, TILE))
        return a.reshape(TILES, 128)

    row_bounds = columns_of(per_row(rows_at * 2**SPAN_BITS + rows_at - rows_from))
    key_parts, windows = [], []
    for first, count in ((0, 24), (24, 8)):
        part = key_at[:, first : first + count].reshape(TILES, count * TILE)
        tile_first = jnp.min(part, axis=1)
        tile_last = jnp.max(part, axis=1)
        low = jnp.sum((tile_last[None, :] < first_needed[:, None]).astype(jnp.int32), axis=1)
        high = jnp.sum((tile_first[None, :] <= last_needed[:, None]).astype(jnp.int32), axis=1)
        key_parts.append(part)
        windows.append((low, high))
    cosine, sine, row_bounds, key_parts, windows = lax.optimization_barrier(
        (cosine, sine, row_bounds, key_parts, windows)
    )

    kv_near = project_kv(near_rows, w_key, w_value, cosine, sine, TOK)
    kv_other, kv_mine = finish_kv(
        core_arg, far_rows, w_key, w_value, cosine, sine, rank_row, (kv_own, kv_near)
    )
    kv_partner = swap_cores(kv_other)
    chip = jnp.concatenate([kv_mine[None], kv_partner[None]], axis=0)

    back = send(chip, first_axis(1))
    ahead = send(chip, first_axis(-1))
    chip_b = send(chip, second_axis(1))
    chip_a = send(chip, second_axis(-1))
    far = send(ahead, first_axis(-1))
    back_b = send(back, second_axis(1))
    ahead_a = send(ahead, second_axis(-1))
    ahead_b = send(ahead, second_axis(1))
    back_a = send(back, second_axis(-1))
    end_b = send(far, second_axis(1))
    end_a = send(far, second_axis(-1))
    chip_f = send(chip_b, second_axis(1))
    back_f = send(back_b, second_axis(1))
    ahead_f = send(ahead_a, second_axis(-1))
    end_f = send(end_a, second_axis(-1))

    pieces = (*own_rows, *near_rows, *far_rows)
    q_other = project_q(core_arg, pieces, w_query, cosine, sine, rank_row, False)
    q_mine = project_q(core_arg, pieces, w_query, cosine, sine, rank_row, True)
    q_partner = swap_cores(q_other)
    queries = (q_mine, q_partner)

    near_kv = (chip, back, ahead, far)
    near_kv += (chip_b, back_b, ahead_b, end_b, chip_a, back_a, ahead_a, end_a)
    state = attend(
        windows[0], queries, key_parts[0], row_bounds, near_kv, None, 4
    )
    state = attend(
        windows[1],
        queries,
        key_parts[1],
        row_bounds,
        (chip_f, back_f, ahead_f, end_f),
        state,
        8,
        w_output,
    )
    mine, partner, w_near = state
    other = swap_cores(partner)

    def plus(a, b):
        return a.astype(jnp.float32) + b.astype(jnp.float32)

    ways = (along_z(1), along_z(1), along_z(-1), along_z(-1))
    moving = products(
        core_arg, rank_row, mine, other, w_near, ((1, 0), (1, 1), (2, 2), (2, 3))
    )
    moving = [send(a, way) for a, way in zip(moving, ways)]
    terms = products(
        core_arg,
        rank_row,
        mine,
        other,
        w_near,
        tuple(
            (block, side)
            for blocks in ((3, 3, 3, 3), (2, 2, 1, 1), (0, 0, 0, 0))
            for side, block in enumerate(blocks)
        ),
    )
    for first in (0, 4):
        moving = [
            send(plus(a, b).astype(jnp.bfloat16), way)
            for a, b, way in zip(moving, terms[first : first + 4], ways)
        ]
    attended = jnp.concatenate([plus(a, b) for a, b in zip(moving, terms[8:])], axis=1)
    return (tokens.astype(jnp.float32) + attended).astype(jnp.bfloat16)


def solution(mesh):
    placed = (
        P(("dp", "tp"), None),
        P(),
        P(None, "tp"),
        P(None, "tp"),
        P(None, "tp"),
        P("tp", None),
        P(),
        P(),
    )
    return jax.shard_map(
        layer, mesh=mesh, in_specs=placed, out_specs=P(("dp", "tp"), None), check_vma=False
    )
```

```python
import functools

import jax
import jax.numpy as jnp
from jax import lax
from jax.experimental import pallas as pl
from jax.experimental.pallas import tpu as pltpu
from jax.sharding import PartitionSpec as P


HEAD_DIM = 128
NY, NX, NZ = 4, 4, 4
GROUPS = 32
TOK = 128
ROWS = NZ * TOK
TILE = 16
SPAN_BITS = 9
TILES = ROWS // TILE
LOG2E = 1.4426950408889634

rope_base = 500000.0
norm_eps = 1e-05
score_floor = -1e30

AXES = ("dp", "tp")
VMEM = pltpu.VMEM


def group_of(y, x, core):
    return ((y % NY) * NX + (x % NX)) * 2 + core


def pairs(move):
    out = []
    for y in range(NY):
        for x in range(NX):
            for core in range(2):
                for z in range(NZ):
                    y2, x2, core2, z2 = move(y, x, core, z)
                    out.append(
                        (group_of(y, x, core) * NZ + z, group_of(y2, x2, core2) * NZ + z2 % NZ)
                    )
    return out


def first_axis(s):
    return pairs(
        lambda y, x, core, z: (y, x + s, core, z) if core == 0 else (y + s, x, core, z)
    )


def second_axis(s):
    return pairs(
        lambda y, x, core, z: (y + s, x, core, z) if core == 0 else (y, x + s, core, z)
    )


def along_z(s):
    return pairs(lambda y, x, core, z: (y, x, core, z + s))


def send(array, moves):
    return lax.ppermute(array, AXES, moves)


def swap_cores(array):
    return send(array, pairs(lambda y, x, core, z: (y, x, 1 - core, z)))


def cost(flops, nbytes, exps=0):
    return pl.CostEstimate(flops=int(flops), bytes_accessed=int(nbytes), transcendentals=int(exps))


def whole():
    return pl.BlockSpec(memory_space=VMEM)


def scalars():
    return pl.BlockSpec(memory_space=pltpu.SMEM)


def small():
    return pltpu.CompilerParams(vmem_limit_bytes=8 * 2**20)


def norm_kernel(tokens_ref, gain_ref, low_ref, high_ref):
    gain = gain_ref[...]
    half = low_ref.shape[0]

    for first, out_ref in ((0, low_ref), (half, high_ref)):

        def chunk(i, _):
            at = pl.multiple_of(i * 16, 16)
            rows = tokens_ref[pl.ds(first + at, 16), :].astype(jnp.float32)
            scale = lax.rsqrt(jnp.mean(rows * rows, axis=1, keepdims=True) + norm_eps)
            out_ref[pl.ds(at, 16), :] = (rows * scale * gain).astype(jnp.bfloat16)
            return 0

        lax.fori_loop(0, half // 16, chunk, 0)


def normalise(tokens, gain):
    rows, width = tokens.shape
    return pl.pallas_call(
        norm_kernel,
        out_shape=[jax.ShapeDtypeStruct((rows // 2, width), jnp.bfloat16)] * 2,
        in_specs=[whole(), whole()],
        out_specs=[whole(), whole()],
        compiler_params=small(),
        cost_estimate=cost(rows * width * 5, rows * width * 4),
    )(tokens, gain.reshape(1, width))


def as_column(row):
    return jnp.broadcast_to(row, (128, 128)).T


def order_kernel(packed_ref, out_ref):
    lane = lax.broadcasted_iota(jnp.int32, (128, 128), 1).astype(jnp.float32)
    blocks = ROWS // 128

    def one_group(g, _):
        row = packed_ref[pl.ds(g, 1), :]
        pieces = [row[:, i * 128 : (i + 1) * 128] for i in range(blocks)]
        sums = [jnp.zeros((128, 128), jnp.float32) for _ in range(blocks)]
        for j in range(blocks):
            column = as_column(pieces[j])
            below = jnp.zeros((128, 128), jnp.float32)
            for i in range(blocks):
                below = below + jnp.where(pieces[i] < column, 1.0, 0.0)
            rank = jnp.sum(below, axis=1, keepdims=True)
            for i in range(blocks):
                sums[i] = sums[i] + jnp.where(rank == lane + float(i * 128), column, 0.0)
        out_ref[pl.ds(g, 1), :] = jnp.concatenate(
            [jnp.sum(s, axis=0, keepdims=True) for s in sums], axis=1
        )
        return 0

    lax.fori_loop(0, GROUPS, one_group, 0)


def order_groups(packed):
    return pl.pallas_call(
        order_kernel,
        out_shape=jax.ShapeDtypeStruct((GROUPS, ROWS), jnp.float32),
        in_specs=[whole()],
        out_specs=whole(),
        compiler_params=small(),
        cost_estimate=cost(6 * GROUPS * ROWS * ROWS, 8 * GROUPS * ROWS),
    )(packed)


def column_kernel(packed_ref, out_ref):
    def one(u, _):
        at = pl.ds(pl.multiple_of(u * 128, 128), 128)
        out_ref[at, :] = as_column(packed_ref[pl.ds(u, 1), :])
        return 0

    lax.fori_loop(0, TILES, one, 0)


def columns_of(packed):
    return pl.pallas_call(
        column_kernel,
        out_shape=jax.ShapeDtypeStruct((TILES * 128, 128), jnp.int32),
        in_specs=[whole()],
        out_specs=whole(),
        compiler_params=small(),
        cost_estimate=cost(TILES * 128 * 128 * 32, TILES * 128 * 512),
    )(packed)


def turn(head, cosine, sine):
    return head * cosine + pltpu.roll(head, HEAD_DIM // 2, 1) * sine


def stacked(refs):
    if len(refs) == 1:
        return refs[0][...]
    return jnp.concatenate([ref[...] for ref in refs], axis=0)


def keys_and_values(rows, wk_ref, wv_ref, cosine, sine):
    keys = jnp.dot(rows, wk_ref[...], preferred_element_type=jnp.float32)
    values = jnp.dot(rows, wv_ref[...], preferred_element_type=jnp.float32)
    out = []
    for head in range(2):
        at = slice(head * HEAD_DIM, (head + 1) * HEAD_DIM)
        key = turn(keys[:, at], cosine, sine)
        out.append(jnp.concatenate([key, values[:, at]], axis=1).astype(jnp.bfloat16))
    return out


def kv_kernel(parts, first, *refs):
    wk_ref, wv_ref, cos_ref, sin_ref, out_ref = refs[parts:]
    rows = stacked(refs[:parts])
    at = slice(first, first + rows.shape[0])
    for head, block in enumerate(
        keys_and_values(rows, wk_ref, wv_ref, cos_ref[at, :], sin_ref[at, :])
    ):
        out_ref[head] = block


def project_kv(pieces, w_key, w_value, cosine, sine, first):
    width = w_key.shape[0]
    rows = sum(p.shape[0] for p in pieces)
    return pl.pallas_call(
        functools.partial(kv_kernel, len(pieces), first),
        out_shape=jax.ShapeDtypeStruct((2, rows, 256), jnp.bfloat16),
        in_specs=[whole()] * (len(pieces) + 4),
        out_specs=whole(),
        compiler_params=small(),
        cost_estimate=cost(2 * rows * width * 512, width * 1024 + rows * width * 2),
    )(*pieces, w_key, w_value, cosine, sine)


def sorting(rank_row):
    slot = lax.broadcasted_iota(jnp.int32, (ROWS, ROWS), 0)
    return (slot == rank_row).astype(jnp.bfloat16)


def last_kv_kernel(parts, core_ref, *refs):
    wk_ref, wv_ref, cos_ref, sin_ref, rank_ref = refs[parts : parts + 5]
    done_refs, (other_ref, mine_ref) = refs[parts + 5 : -3], refs[-3:-1]
    last_ref = refs[-1]
    rows = stacked(refs[:parts])
    at = slice(ROWS - rows.shape[0], ROWS)
    for head, block in enumerate(
        keys_and_values(rows, wk_ref, wv_ref, cos_ref[at, :], sin_ref[at, :])
    ):
        last_ref[head] = block
    pick = sorting(rank_ref[...])
    core = core_ref[0]
    for head, out_ref in ((1 - core, other_ref), (core, mine_ref)):
        rows = jnp.concatenate([ref[head] for ref in (*done_refs, last_ref)], axis=0)
        out_ref[...] = jnp.dot(pick, rows, preferred_element_type=jnp.float32).astype(jnp.bfloat16)


def finish_kv(core, pieces, w_key, w_value, cosine, sine, rank_row, done):
    width = w_key.shape[0]
    rows = sum(p.shape[0] for p in pieces)
    shape = jax.ShapeDtypeStruct((ROWS, 256), jnp.bfloat16)
    return pl.pallas_call(
        functools.partial(last_kv_kernel, len(pieces)),
        out_shape=(shape, shape),
        in_specs=[scalars()] + [whole()] * (len(pieces) + 5 + len(done)),
        out_specs=(whole(), whole()),
        scratch_shapes=[pltpu.VMEM((2, rows, 256), jnp.bfloat16)],
        compiler_params=small(),
        cost_estimate=cost(2 * rows * width * 512, width * 1024 + rows * width * 2),
    )(core, *pieces, w_key, w_value, cosine, sine, rank_row, *done)


def q_kernel(parts, mine, core_ref, *refs):
    w_ref, cos_ref, sin_ref, rank_ref, out_ref, turned_ref = refs[parts:]
    half = core_ref[0] if mine else 1 - core_ref[0]
    for block in range(NZ):
        rows = stacked(refs[2 * block : 2 * block + 2])
        at = slice(block * TOK, (block + 1) * TOK)
        cosine, sine = cos_ref[at, :], sin_ref[at, :]
        for first in range(0, 512, 256):
            columns = pl.ds(pl.multiple_of(half * 512 + first, 256), 256)
            both = jnp.dot(rows, w_ref[:, columns], preferred_element_type=jnp.float32)
            turned = jnp.concatenate(
                [turn(both[:, :HEAD_DIM], cosine, sine), turn(both[:, HEAD_DIM:], cosine, sine)],
                axis=1,
            )
            turned_ref[at, first : first + 256] = turned.astype(jnp.bfloat16)
    out_ref[...] = jnp.dot(
        sorting(rank_ref[...]), turned_ref[...], preferred_element_type=jnp.float32
    ).astype(jnp.bfloat16)


def project_q(core, pieces, w_query, cosine, sine, rank_row, mine):
    width = w_query.shape[0]
    return pl.pallas_call(
        functools.partial(q_kernel, len(pieces), mine),
        out_shape=jax.ShapeDtypeStruct((ROWS, 512), jnp.bfloat16),
        in_specs=[scalars()] + [whole()] * (len(pieces) + 4),
        out_specs=whole(),
        scratch_shapes=[pltpu.VMEM((ROWS, 512), jnp.bfloat16)],
        compiler_params=small(),
        cost_estimate=cost(2 * ROWS * width * 512, width * 1024 + ROWS * width * 2),
    )(core, *pieces, w_query, cosine, sine, rank_row)


def attend_kernel(opening, closing, batch, count, low_ref, high_ref, *refs):
    q_refs, refs = refs[:2], refs[2:]
    key_at_ref, bound_ref = refs[:2]
    kv_refs, refs = refs[2 : 2 + count], refs[2 + count :]
    if not opening:
        old_ref, refs = refs[0], refs[1:]
    if closing:
        w_from, out_refs, (w_to, state_ref, arrived) = refs[0], refs[1:3], refs[3:]
        copy = pltpu.make_async_copy(w_from, w_to, arrived)
        copy.start()
    else:
        (state_ref,) = refs

    scale = HEAD_DIM ** (-0.5) * LOG2E

    def at(u, size):
        return pl.ds(pl.multiple_of(u * size, size), size)

    def queries(u):
        return jnp.concatenate(
            [
                ref[at(u, TILE), h * HEAD_DIM : (h + 1) * HEAD_DIM]
                for ref in q_refs
                for h in range(4)
            ],
            axis=0,
        )

    def keys(t):
        return jnp.concatenate(
            [ref[:, at(t, TILE), :].reshape(-1, 256) for ref in kv_refs], axis=0
        )

    def spread(a, wide=1):
        a = jnp.broadcast_to(a, (128, 128))
        return a if wide == 1 else jnp.concatenate([a] * wide, axis=1)

    def update(us, kvs, key_ats, states):
        wide = kvs[0].shape[0] // 128
        scores = [
            lax.dot_general(
                queries(u),
                kv[:, :HEAD_DIM],
                (((1,), (1,)), ((), ())),
                preferred_element_type=jnp.float32,
            )
            for u, kv in zip(us, kvs)
        ]
        masked = []
        for u, score, key_at in zip(us, scores, key_ats):
            bound = bound_ref[at(u, 128), :]
            upper = bound >> SPAN_BITS
            lower = upper - (bound & (2**SPAN_BITS - 1))
            allowed = (key_at <= spread(upper, wide)) & (key_at >= spread(lower, wide))
            masked.append(jnp.where(allowed, score, score_floor))
        peaks = [spread(jnp.max(m, axis=1, keepdims=True)) for m in masked]
        peaks = [p if st is None else jnp.maximum(p, st[0]) for p, st in zip(peaks, states)]
        weights = [jnp.exp2((m - spread(p, wide)) * scale) for m, p in zip(masked, peaks)]
        totals = [spread(jnp.sum(w, axis=1, keepdims=True)) for w in weights]
        mixes = [
            jnp.dot(w.astype(jnp.bfloat16), kv[:, HEAD_DIM:], preferred_element_type=jnp.float32)
            for w, kv in zip(weights, kvs)
        ]
        out = []
        for peak, total, mixed, st in zip(peaks, totals, mixes, states):
            if st is not None:
                keep = jnp.exp2((st[0] - peak) * scale)
                total = total + st[1] * keep
                mixed = mixed + st[2] * keep
            out.append((peak, total, mixed))
        return out

    def load(ref, u):
        return tuple(ref[at(u, 128), i * 128 : (i + 1) * 128] for i in range(3))

    def save(u, state):
        for i, part in enumerate(state):
            state_ref[at(u, 128), i * 128 : (i + 1) * 128] = part

    def write(u, state):
        _, total, mixed = state
        context = (mixed / total).astype(jnp.bfloat16)
        for i, ref in enumerate(out_refs):
            for h in range(4):
                block = (i * 4 + h) * TILE
                ref[at(u, TILE), h * HEAD_DIM : (h + 1) * HEAD_DIM] = context[block : block + TILE]

    def finish(us, states):
        for u, state in zip(us, states):
            save(u, state)
            if closing:
                write(u, state)

    def some(i, _):
        us = [batch * i + n for n in range(batch)]
        kvs, key_ats = [], []
        for u in us:
            low, high = low_ref[u], high_ref[u]
            t0 = jnp.minimum(low, TILES - 1)
            t1 = jnp.minimum(low + 1, TILES - 1)
            at0 = jnp.where(low < high, key_at_ref[pl.ds(t0, 1), :], -1)
            at1 = jnp.where(low + 1 < high, key_at_ref[pl.ds(t1, 1), :], -1)
            kvs.append(jnp.concatenate([keys(t0), keys(t1)], axis=0))
            key_ats.append(jnp.concatenate([at0, at1], axis=1))
        states = [None if opening else load(old_ref, u) for u in us]
        finish(us, update(us, kvs, key_ats, states))
        return 0

    lax.fori_loop(0, TILES // batch, some, 0)

    def rest(u, _):
        def more(t, _):
            key_at = key_at_ref[pl.ds(t, 1), :]
            finish([u], update([u], [keys(t)], [key_at], [load(state_ref, u)]))
            return 0

        return lax.fori_loop(low_ref[u] + 2, high_ref[u], more, 0)

    lax.fori_loop(0, TILES, rest, 0)
    if closing:
        copy.wait()


def attend(bounds, queries, key_at, row_bounds, kvs, state, batch, resident=None):
    opening, closing = state is None, resident is not None
    running = jax.ShapeDtypeStruct((TILES * 128, 384), jnp.float32)
    operands = [*bounds, *queries, key_at, row_bounds, *kvs, *(() if opening else (state,))]
    in_specs = [scalars(), scalars()] + [whole()] * (len(operands) - 2)
    out_shape, out_specs, scratch = running, whole(), ()
    if closing:
        operands.append(resident)
        in_specs.append(pl.BlockSpec(memory_space=pltpu.HBM))
        context = jax.ShapeDtypeStruct((ROWS, 512), jnp.bfloat16)
        out_shape = [context, context, jax.ShapeDtypeStruct(resident.shape, resident.dtype)]
        out_specs = [whole()] * 3
        scratch = [pltpu.VMEM((TILES * 128, 384), jnp.float32), pltpu.SemaphoreType.DMA]
    rows = sum(kv.shape[0] for kv in kvs) * TILE * 2
    return pl.pallas_call(
        functools.partial(attend_kernel, opening, closing, batch, len(kvs)),
        out_shape=out_shape,
        in_specs=in_specs,
        out_specs=out_specs,
        scratch_shapes=scratch,
        compiler_params=pltpu.CompilerParams(vmem_limit_bytes=(29 if closing else 8) * 2**20),
        cost_estimate=cost(TILES * 128 * rows * 512, 10e6, TILES * 128 * rows),
    )(*operands)


def unsort(rank_row, block, parts):
    slot = lax.broadcasted_iota(jnp.int32, (TOK, ROWS), 1)
    rank = as_column(rank_row[:, block * TOK : (block + 1) * TOK])
    pick = (slot == jnp.concatenate([rank] * (ROWS // 128), axis=1)).astype(jnp.bfloat16)
    return [
        jnp.dot(pick, part[...], preferred_element_type=jnp.float32).astype(jnp.bfloat16)
        for part in parts
    ]


def product_kernel(wanted, core_ref, rank_ref, mine_ref, other_ref, w_ref, *out_refs):
    core = core_ref[0]
    mine_at = pl.ds(pl.multiple_of(core * 512, 512), 512)
    other_at = pl.ds(pl.multiple_of((1 - core) * 512, 512), 512)
    part = w_ref.shape[1] // 4
    rank = rank_ref[...]
    rows = {}
    for block, _ in wanted:
        if block not in rows:
            rows[block] = unsort(rank, block, (mine_ref, other_ref))
    for side in range(4):
        group = [(i, block) for i, (block, s) in enumerate(wanted) if s == side]
        if not group:
            continue
        mine = jnp.concatenate([rows[block][0] for _, block in group], axis=0)
        other = jnp.concatenate([rows[block][1] for _, block in group], axis=0)
        at = slice(side * part, (side + 1) * part)
        product = jnp.dot(
            mine, w_ref[mine_at, at], preferred_element_type=jnp.float32
        ) + jnp.dot(other, w_ref[other_at, at], preferred_element_type=jnp.float32)
        for n, (i, _) in enumerate(group):
            out_refs[i][...] = product[n * TOK : (n + 1) * TOK].astype(jnp.bfloat16)


def products(core, rank_row, mine, other, w_output, wanted):
    width = w_output.shape[1]
    shape = jax.ShapeDtypeStruct((TOK, width // 4), jnp.bfloat16)
    return pl.pallas_call(
        functools.partial(product_kernel, wanted),
        out_shape=[shape] * len(wanted),
        in_specs=[scalars()] + [whole()] * 4,
        out_specs=[whole()] * len(wanted),
        compiler_params=small(),
        cost_estimate=cost(TOK * 512 * width * len(wanted), 1024 * width * 2),
    )(core, rank_row, mine, other, w_output)


def document_start(position, starts):
    reached = starts <= position[..., None]
    return jnp.max(jnp.where(reached, starts, 0), axis=-1)


def layer(tokens, norm_gain, w_query, w_key, w_value, w_output, doc_lengths, pack_index):
    group = lax.axis_index("dp")
    z = lax.axis_index("tp")
    core = group % 2
    chip_x = (group // 2) % NX
    chip_y = group // (2 * NX)
    core_arg = core.astype(jnp.int32).reshape(1)

    own_low, own_high = normalise(tokens, norm_gain)
    below_low = send(own_low, along_z(1))
    above_high = send(own_high, along_z(-1))
    below_high = send(own_high, along_z(1))
    above_low = send(own_low, along_z(-1))
    far_low = send(below_low, along_z(1))
    far_high = send(above_high, along_z(-1))
    own_rows = (own_low, own_high)
    near_rows = (below_low, below_high, above_low, above_high)
    far_rows = (far_low, far_high)

    number = jnp.arange(doc_lengths.shape[0], dtype=jnp.int32)
    starts = jnp.sum(jnp.where(number[None, :] < number[:, None], doc_lengths[None, :], 0), axis=1)
    by_group = pack_index.reshape(GROUPS, NZ, TOK)
    own = lax.dynamic_index_in_dim(by_group, group, 0, keepdims=False)
    order = (z + jnp.array([0, NZ - 1, 1, 2], jnp.int32)) % NZ
    packed = jnp.take(own, order, axis=0).reshape(ROWS)
    place = packed - document_start(packed, starts)
    rank_row = jnp.sum((packed[:, None] < packed[None, :]).astype(jnp.int32), axis=0)
    rank_row = rank_row.reshape(1, ROWS)
    half_dim = HEAD_DIM // 2
    frequency = rope_base ** (-2.0 * jnp.arange(half_dim, dtype=jnp.float32) / HEAD_DIM)
    angles = place.astype(jnp.float32)[:, None] * frequency[None, :]
    cosine, sine = jnp.cos(angles), jnp.sin(angles)
    cosine = jnp.concatenate([cosine, cosine], axis=1)
    sine = jnp.concatenate([-sine, sine], axis=1)

    kv_own = project_kv(own_rows, w_key, w_value, cosine, sine, 0)

    ordered = order_groups(pack_index.reshape(GROUPS, ROWS).astype(jnp.float32))
    ordered = ordered.astype(jnp.int32)
    offsets = jnp.array([0, -1, 1, 2], jnp.int32)
    outer, inner = offsets[:, None, None], offsets[None, :, None]
    which = (core + jnp.arange(2, dtype=jnp.int32)) % 2
    dy = jnp.where(core == 0, outer, inner)
    dx = jnp.where(core == 0, inner, outer)
    source = (((chip_y + dy) % NY) * NX + (chip_x + dx) % NX) * 2 + which[None, None, :]
    key_at = jnp.take(ordered, source.reshape(GROUPS), axis=0)
    key_at = key_at.reshape(GROUPS, TILES, TILE).transpose(1, 0, 2)
    rows_at = jnp.take(ordered, jnp.stack([group, group + 1 - 2 * core]), axis=0)
    rows_from = document_start(rows_at, starts)
    rows_at = rows_at.reshape(2, TILES, TILE)
    rows_from = rows_from.reshape(2, TILES, TILE)
    first_needed = jnp.min(rows_from, axis=(0, 2))
    last_needed = jnp.max(rows_at, axis=(0, 2))

    def per_row(a):
        a = jnp.broadcast_to(a.transpose(1, 0, 2)[:, :, None, :], (TILES, 2, 4, TILE))
        return a.reshape(TILES, 128)

    row_bounds = columns_of(per_row(rows_at * 2**SPAN_BITS + rows_at - rows_from))
    key_parts, windows = [], []
    for first, count in ((0, 24), (24, 8)):
        part = key_at[:, first : first + count].reshape(TILES, count * TILE)
        tile_first = jnp.min(part, axis=1)
        tile_last = jnp.max(part, axis=1)
        low = jnp.sum((tile_last[None, :] < first_needed[:, None]).astype(jnp.int32), axis=1)
        high = jnp.sum((tile_first[None, :] <= last_needed[:, None]).astype(jnp.int32), axis=1)
        key_parts.append(part)
        windows.append((low, high))
    cosine, sine, row_bounds, key_parts, windows = lax.optimization_barrier(
        (cosine, sine, row_bounds, key_parts, windows)
    )

    kv_near = project_kv(near_rows, w_key, w_value, cosine, sine, TOK)
    kv_other, kv_mine = finish_kv(
        core_arg, far_rows, w_key, w_value, cosine, sine, rank_row, (kv_own, kv_near)
    )
    kv_partner = swap_cores(kv_other)
    chip = jnp.concatenate([kv_mine[None], kv_partner[None]], axis=0)

    back = send(chip, first_axis(1))
    ahead = send(chip, first_axis(-1))
    chip_b = send(chip, second_axis(1))
    chip_a = send(chip, second_axis(-1))
    far = send(ahead, first_axis(-1))
    back_b = send(back, second_axis(1))
    ahead_a = send(ahead, second_axis(-1))
    ahead_b = send(ahead, second_axis(1))
    back_a = send(back, second_axis(-1))
    end_b = send(far, second_axis(1))
    end_a = send(far, second_axis(-1))
    chip_f = send(chip_b, second_axis(1))
    back_f = send(back_b, second_axis(1))
    ahead_f = send(ahead_a, second_axis(-1))
    end_f = send(end_a, second_axis(-1))

    pieces = (*own_rows, *near_rows, *far_rows)
    q_other = project_q(core_arg, pieces, w_query, cosine, sine, rank_row, False)
    q_mine = project_q(core_arg, pieces, w_query, cosine, sine, rank_row, True)
    q_partner = swap_cores(q_other)
    queries = (q_mine, q_partner)

    near_kv = (chip, back, ahead, far)
    near_kv += (chip_b, back_b, ahead_b, end_b, chip_a, back_a, ahead_a, end_a)
    state = attend(
        windows[0], queries, key_parts[0], row_bounds, near_kv, None, 4
    )
    state = attend(
        windows[1],
        queries,
        key_parts[1],
        row_bounds,
        (chip_f, back_f, ahead_f, end_f),
        state,
        8,
        w_output,
    )
    mine, partner, w_near = state
    other = swap_cores(partner)

    def plus(a, b):
        return a.astype(jnp.float32) + b.astype(jnp.float32)

    ways = (along_z(1), along_z(-1)) * 2
    first = products(core_arg, rank_row, mine, other, w_near, ((1, 0), (2, 2)))
    early = [send(a, way) for a, way in zip(first, ways)]
    sides = (0, 2, 1, 3)
    terms = products(
        core_arg,
        rank_row,
        mine,
        other,
        w_near,
        ((1, 1), (2, 3))
        + tuple(
            (block, side)
            for blocks in ((3, 3, 3, 3), (2, 1, 2, 1), (0, 0, 0, 0))
            for side, block in zip(sides, blocks)
        ),
    )
    late = [send(a, way) for a, way in zip(terms[:2], ways)]
    moving = early + late
    for first in (2, 6):
        moving = [
            send(plus(a, b).astype(jnp.bfloat16), way)
            for a, b, way in zip(moving, terms[first : first + 4], ways)
        ]
    attended = [plus(a, b) for a, b in zip(moving, terms[10:])]
    attended = jnp.concatenate([attended[n] for n in (0, 2, 1, 3)], axis=1)
    return (tokens.astype(jnp.float32) + attended).astype(jnp.bfloat16)


def solution(mesh):
    placed = (
        P(("dp", "tp"), None),
        P(),
        P(None, "tp"),
        P(None, "tp"),
        P(None, "tp"),
        P("tp", None),
        P(),
        P(),
    )
    return jax.shard_map(
        layer, mesh=mesh, in_specs=placed, out_specs=P(("dp", "tp"), None), check_vma=False
    )
```
